128 devices in a mesh: dp: 8 (over y, x_lo), expert: 16 (over x_hi, z, core).
Axes of the slice: x: 4 (x_hi: 2, x_lo: 2; x = x_hi * 2 + x_lo), y: 4, z: 4, core: 2. Of those that a mesh axis runs over, the one named last changes fastest.
Arguments:
- tokens: bfloat16 [40960, 2048], P(('dp', 'expert')), may hold values from -24 to 24
- out_grad: bfloat16 [40960, 2048], P(('dp', 'expert')), may hold values from -24 to 24
- expert_ids: int32 [40960, 2], P(('dp', 'expert')), may hold values from 0 to 15, all different within a row; in each aligned block of 320 rows (0 to 319, 320 to 639, ...) at most 60 rows name the same one
- route_weight: bfloat16 [40960, 2], P(('dp', 'expert')), may hold values from 0.099609375 to 1
- w_gate: bfloat16 [16, 2048, 768], P('expert', 'dp'), may hold values from -0.125 to 0.125
- w_up: bfloat16 [16, 2048, 768], P('expert', 'dp'), may hold values from -0.125 to 0.125
- w_down: bfloat16 [16, 768, 2048], P('expert', None, 'dp'), may hold values from -0.21875 to 0.21875
Outputs:
- token_grad: bfloat16 [40960, 2048], P(('dp', 'expert'))
- route_grad: bfloat16 [40960, 2], P(('dp', 'expert'))
- gate_grad: bfloat16 [16, 2048, 768], P('expert', 'dp')
- up_grad: bfloat16 [16, 2048, 768], P('expert', 'dp')
- down_grad: bfloat16 [16, 768, 2048], P('expert', None, 'dp')
The draws below stay inside these ranges and needn't reach their ends.
Inputs may be any that keep to these rules, and one draw needn't show every extreme that they name: `expert_ids`: each row names 2 different experts. In the rows of one device no expert is named more than 60 times, a bound that some block reaches in some device.
All inputs are finite; a program needn't handle non-finite values.
Results may differ from the reference program's by a relative error of at most 0.014.
Values may be sent and summed in bfloat16 or wider, within the bound.
A program may use at most 128 MiB of HBM per device.

```python
import math
import jax
import jax.numpy as jnp
import numpy as np
from jax import lax

D = 2048
FF = 768
TOP_WIN = 2
TOK_DEV = 320
EXPERTS_WIN = 16
CAP = 60
TOKENS = 40960
N_DP = 8
N_EXPERT = 16


def with_spikes(result, key, source, target, blocks, factor):
    owner, partner = [(jnp.arange(result.shape[axis_at]) // (result.shape[axis_at] // blocks)).reshape([-1 if axis == axis_at else 1 for axis in range(result.ndim)]) for axis_at in (source, target)]
    chosen = jax.random.permutation(key, blocks)[partner]
    strong = (owner == chosen) | (owner == (partner + blocks // 2) % blocks)
    return jnp.where(strong, factor * result, result)


def steps_of(rng, shape, pieces, smallest, largest):
    loudness = 1.0
    for dim, shards_of in pieces:
        heights = jax.random.uniform(jax.random.fold_in(jax.random.fold_in(rng, 6), dim), (shards_of,), jnp.float32, smallest / len(pieces), largest / len(pieces))
        loudness = loudness * jnp.repeat(jnp.exp(heights), shape[dim] // shards_of).reshape((-1,) + (1,) * (len(shape) - 1 - dim))
    return loudness


def routed_block(rng, own, number, rows, number_of, top, limit, slope):
    order = jax.random.permutation(rng, number_of)
    heavy_load, common = portions_of(number_of, rows * top, limit, slope, True), portions_of(number_of, rows * top, limit, slope, False)
    places = jnp.arange(number_of)

    def named(tallies, offset_by):
        used = int((tallies > 0).sum())
        fixed = max(1, used // 4)
        shifted = fixed + (places - fixed + offset_by * (used - fixed)) % max(1, number_of - fixed)
        return jnp.zeros((number_of,), jnp.int32).at[order[jnp.where(places < fixed, places, shifted)]].set(jnp.asarray(tallies, jnp.int32))

    tallies = jnp.where(number % 4 == 0, named(heavy_load, number // 4), named(common, number - number // 4 - 1))
    mixed = jax.random.permutation(jax.random.fold_in(own, 3), number_of)
    donor, taker = mixed[0:number_of // 2 * 2:2], mixed[1:number_of // 2 * 2:2]
    slack = jnp.minimum(tallies[donor] - 1, limit - tallies[taker]) // 2
    slack = jnp.where((donor == order[0]) | (taker == order[0]) | (tallies[taker] == 0), 0, jnp.maximum(slack, 0))
    shifted = jax.random.randint(jax.random.fold_in(own, 4), (number_of // 2,), 0, 1 << 20) % (slack + 1)
    tallies = tallies.at[donor].add(-shifted).at[taker].add(shifted)
    members = jnp.searchsorted(jnp.cumsum(tallies), jnp.arange(rows * top), side="right").astype(jnp.int32)
    listing = members.reshape(top, rows).T
    listing = listing[jax.random.permutation(jax.random.fold_in(own, 1), rows)]
    offset_by = jax.random.randint(jax.random.fold_in(own, 2), (rows, 1), 0, top)
    return jnp.take_along_axis(listing, (jnp.arange(top)[None, :] + offset_by) % top, axis=1)


def portions_of(count, total, most, lean, full):
    loads = [(1 << 20) // math.isqrt(standing ** lean) + 1 for standing in range(1, count + 1)]
    largest = most if full else min(most, max(-(-total // count), total * loads[0] // sum(loads)))
    least = 1 if total - largest >= count - 1 else 0
    given, rest = [largest] + [least] * (count - 1), total - largest - least * (count - 1)
    while rest > 0:
        movable = [i for i in range(1, count) if given[i] < largest] or [i for i in range(1, count) if given[i] < most]
        pool, left = sum([loads[i] for i in movable]), rest
        for i in movable:
            more = min(most - given[i], max(1, left * loads[i] // pool), rest)
            given[i] = given[i] + more
            rest = rest - more
    return np.array(given)


def noise(stream_key, extent, scale, most, pieces=(), held_as=jnp.bfloat16):
    result = scale * jax.random.normal(stream_key, extent, jnp.float32)
    if pieces:
        result = result * steps_of(stream_key, extent, pieces, -0.22, 0.18)
    return jnp.clip(result, -most, most).astype(held_as)


def gaussian_with(stream_key, extent, deviation, bound, split, heavy, kind=jnp.bfloat16):
    result = deviation * jax.random.normal(stream_key, extent, jnp.float32)
    if split:
        result = result * steps_of(stream_key, extent, split, -0.22, 0.18)
    return jnp.clip(with_spikes(result, jax.random.fold_in(stream_key, 3), *heavy), -bound, bound).astype(kind)


def setup_inputs(seed: int = 0) -> dict:
    keys = jax.random.split(jax.random.key(seed), 8)
    tokens = gaussian_with(keys[0], (TOKENS, D), 1.0, 24.0, ((0, 128),), (0, 1, 128, 5.5))
    out_grad = gaussian_with(keys[1], (TOKENS, D), 1.0, 24.0, ((0, 128),), (0, 1, 128, 5.5))
    expert_ids_keys = jax.random.split(jax.random.fold_in(keys[2], 1), TOKENS // TOK_DEV)
    expert_ids_turns = jax.random.permutation(jax.random.fold_in(keys[2], 3), TOKENS // TOK_DEV)
    expert_ids = jax.vmap(lambda own, number: routed_block(jax.random.fold_in(keys[2], 2), own, number, TOK_DEV, EXPERTS_WIN, TOP_WIN, CAP, 2))(expert_ids_keys, expert_ids_turns).reshape((TOKENS, TOP_WIN))
    route_weight = jnp.clip(jnp.exp(math.log(1.0) - 2.306499 * jax.random.uniform(keys[3], (TOKENS, TOP_WIN), jnp.float32) ** steps_of(keys[3], (TOKENS, TOP_WIN), ((0, 128),), -0.2, 0.2)), 0.099609375, 1.0).astype(jnp.bfloat16)
    w_gate = noise(keys[4], (EXPERTS_WIN, D, FF), D ** -0.5, 0.125, ((0, 16), (1, 8)))
    w_up = noise(keys[5], (EXPERTS_WIN, D, FF), D ** -0.5, 0.125, ((0, 16), (1, 8)))
    w_down = noise(keys[6], (EXPERTS_WIN, FF, D), FF ** -0.5, 0.21875, ((0, 16), (2, 8)))
    return {"tokens": tokens, "out_grad": out_grad, "expert_ids": expert_ids, "route_weight": route_weight, "w_gate": w_gate, "w_up": w_up, "w_down": w_down}


def reference(tokens, out_grad, expert_ids, route_weight, w_gate, w_up, w_down):
    group_routes = TOK_DEV * N_EXPERT * TOP_WIN
    row_limit = N_EXPERT * CAP
    all_routes = group_routes * N_DP
    all_tokens = TOK_DEV * N_EXPERT * N_DP
    flat_ids = expert_ids.reshape(N_DP, group_routes)
    flat_weights = route_weight.reshape(all_routes)

    def one_group(expert_index, group_index):
        picked = jnp.nonzero(flat_ids[group_index] == expert_index, size=row_limit, fill_value=-1)[0]
        valid = picked >= 0
        route_index = (group_index * group_routes + jnp.maximum(picked, 0)).astype(jnp.int32)
        token_index = (route_index // TOP_WIN).astype(jnp.int32)
        rows_in = jnp.where(valid[:, None], tokens[token_index], jnp.zeros((), tokens.dtype))
        rows_grad = jnp.where(valid[:, None], out_grad[token_index], jnp.zeros((), out_grad.dtype))
        weights = jnp.where(valid, flat_weights[route_index], jnp.zeros((), route_weight.dtype))
        gate_w = w_gate[expert_index]
        up_w = w_up[expert_index]
        down_w = w_down[expert_index]
        gate_value = jnp.dot(rows_in, gate_w, preferred_element_type=jnp.float32)
        up_value = jnp.dot(rows_in, up_w, preferred_element_type=jnp.float32)
        sigmoid_gate = jax.nn.sigmoid(gate_value)
        activated = gate_value * sigmoid_gate
        hidden = (activated * up_value).astype(jnp.bfloat16)
        expert_out = jnp.dot(hidden, down_w, preferred_element_type=jnp.float32)
        route_dot = jnp.sum(expert_out * rows_grad.astype(jnp.float32), axis=1).astype(jnp.bfloat16)
        scaled = (weights.astype(jnp.float32)[:, None] * rows_grad.astype(jnp.float32)).astype(jnp.bfloat16)
        hidden_grad = jnp.dot(scaled, down_w.T, preferred_element_type=jnp.float32)
        gate_delta = (hidden_grad * up_value * sigmoid_gate * (1.0 + gate_value * (1.0 - sigmoid_gate))).astype(jnp.bfloat16)
        up_delta = (hidden_grad * activated).astype(jnp.bfloat16)
        input_grad = (jnp.dot(gate_delta, gate_w.T, preferred_element_type=jnp.float32)
                      + jnp.dot(up_delta, up_w.T, preferred_element_type=jnp.float32)).astype(jnp.bfloat16)
        gate_part = jnp.dot(rows_in.T, gate_delta, preferred_element_type=jnp.float32).astype(jnp.bfloat16)
        up_part = jnp.dot(rows_in.T, up_delta, preferred_element_type=jnp.float32).astype(jnp.bfloat16)
        down_part = jnp.dot(hidden.T, scaled, preferred_element_type=jnp.float32).astype(jnp.bfloat16)
        target = jnp.where(valid, route_index, all_routes).astype(jnp.int32)
        return target, input_grad, route_dot, gate_part, up_part, down_part

    def one_expert(totals, expert_index):
        route_rows, route_dots = totals

        def group_step(group_index):
            return one_group(expert_index, group_index)

        target, input_grad, route_dot, gate_part, up_part, down_part = lax.map(group_step, jnp.arange(N_DP, dtype=jnp.int32))
        flat_target = target.reshape(-1)
        route_rows = route_rows.at[flat_target].set(input_grad.reshape(-1, D), mode="drop")
        route_dots = route_dots.at[flat_target].set(route_dot.reshape(-1), mode="drop")
        gate_sum = jnp.sum(gate_part.astype(jnp.float32), axis=0).astype(jnp.bfloat16)
        up_sum = jnp.sum(up_part.astype(jnp.float32), axis=0).astype(jnp.bfloat16)
        down_sum = jnp.sum(down_part.astype(jnp.float32), axis=0).astype(jnp.bfloat16)
        return (route_rows, route_dots), (gate_sum, up_sum, down_sum)

    start_rows = (jnp.zeros((all_routes, D), jnp.bfloat16), jnp.zeros((all_routes,), jnp.bfloat16))
    finals, grads = lax.scan(one_expert, start_rows, jnp.arange(EXPERTS_WIN, dtype=jnp.int32))
    route_rows, route_dots = finals
    gate_grad, up_grad, down_grad = grads
    token_grad = jnp.sum(route_rows.astype(jnp.float32).reshape(all_tokens, TOP_WIN, D), axis=1).astype(jnp.bfloat16)
    route_grad = route_dots.reshape(all_tokens, TOP_WIN)
    return (token_grad, route_grad, gate_grad, up_grad, down_grad)
```

```python
import jax
import jax.numpy as jnp
from jax import lax
from jax.experimental import pallas as pl
from jax.experimental.pallas import tpu as pltpu
from jax.sharding import PartitionSpec as P

MESH = pl.DeviceIdType.MESH
F32 = jnp.float32
BF16 = jnp.bfloat16
T = 320
D = 2048
FF = 768
CH = 256
NCH = 8
CAP = 60
RB = 128
RV = 2 * CAP
NB = 8
ROWS = NB * RB


def nn(a, b):
    return jnp.dot(a, b, preferred_element_type=F32)


def nt(a, b):
    return lax.dot_general(a, b, (((1,), (1,)), ((), ())), preferred_element_type=F32)


def tn(a, b):
    return lax.dot_general(a, b, (((0,), (0,)), ((), ())), preferred_element_type=F32)


def rem(a, b):
    return lax.rem(a, jnp.int32(b))


def quo(a, b):
    return lax.div(a, jnp.int32(b))


def device(x, y, z, c):
    x, y, z, c = rem(x + 4, 4), rem(y + 4, 4), rem(z + 4, 4), rem(c + 2, 2)
    return {"dp": y * 2 + rem(x, 2), "expert": quo(x, 2) * 8 + z * 2 + c}


def kernel(
    tokens_hbm, grads_hbm, ids_hbm, rw_hbm, wg_hbm, wu_hbm, wd_hbm,
    token_out, route_out, gate_out, up_out, down_out,
    tk, og, ids, rw, meta, xmeta, xr, slots, go, gp, gto, gtp,
    zs, zr, zms, zmr, wg, wu, wd, gd, ud, hwt,
    rag, rau, rad, rbg, rbu, rbd, rxg, rxu, rxd,
    ret, zds, rdot, pown, xr2, ddown, dpar, xdot,
    lsem, osem, xss, xrs, zss, zrs, ags, agr, zts, ztr, xts, xtr,
    ras, rar, rbs, rbr, rxs, rxr,
):
    dp, ex = lax.axis_index("dp"), lax.axis_index("expert")
    x_lo, y = rem(dp, 2), quo(dp, 2)
    x_hi, z, c = quo(ex, 8), rem(quo(ex, 2), 4), rem(ex, 2)
    x = x_hi * 2 + x_lo
    me = z * 2 + c
    xfar = device(x + 2, y, z, c)
    xnear = {"dp": y * 2 + 1 - x_lo, "expert": ex}
    yup, ydn = device(x, y + 1, z, c), device(x, y - 1, z, c)
    ydir = (yup, ydn)

    def peer(b):
        return {"dp": dp, "expert": x_hi * 8 + b}

    def put(src, dst, ss, rs, to):
        return pltpu.make_async_remote_copy(
            src_ref=src, dst_ref=dst, send_sem=ss, recv_sem=rs, device_id=to, device_id_type=MESH
        )

    def got(dst, rs):
        put(dst, dst, rs, rs, xfar).wait_recv()

    def sent(src, ss):
        put(src, src, ss, ss, xfar).wait_send()

    def chunk_col(j):
        k, l = rem(j, 4), quo(j, 4)
        dy = k + quo(k, 2) * (1 - 2 * rem(k, 2))
        owner = 2 * rem(y + dy, 4) + rem(x_lo + l, 2)
        return pl.multiple_of(owner * CH, CH)

    loads = [
        pltpu.make_async_copy(s, d, lsem.at[n])
        for n, (s, d) in enumerate(
            (
                (ids_hbm, ids), (rw_hbm, rw), (tokens_hbm, tk), (grads_hbm, og),
                (wg_hbm, wg.at[0]), (wu_hbm, wu.at[0]), (wd_hbm, wd.at[0]),
            )
        )
    ]
    for cp in loads:
        cp.start()

    def clear(j, _):
        zr[j, :, RV:, :] = jnp.zeros((NB, RB - RV, 2 * CH), BF16)
        ret[j, :, RV:, :] = jnp.zeros((NB, RB - RV, CH), BF16)
        return 0

    lax.fori_loop(0, NCH, clear, 0)
    zmr[:, RV:, :] = jnp.zeros((NB, RB - RV, 128), BF16)
    rdot[:, RV:, :] = jnp.zeros((NB, RB - RV, 128), BF16)

    barrier = pltpu.get_barrier_semaphore()
    greet = [xfar, xnear, yup, ydn] + [peer(rem(me + r, NB)) for r in range(1, NB)]
    for d in greet:
        pl.semaphore_signal(barrier, inc=1, device_id=d, device_id_type=MESH)
    for cp in loads:
        cp.wait()

    lane = lax.broadcasted_iota(jnp.int32, (T, 128), 1)
    id0, id1 = ids[:, 0:1], ids[:, 1:2]
    w0, w1 = rw[:, 0:1].astype(F32), rw[:, 1:2].astype(F32)
    weight_of = jnp.where(lane == id0, w0, 0.0) + jnp.where(lane == id1, w1, 0.0)
    named = jnp.where((lane - 16 == id0) | (lane - 16 == id1), 1.0, 0.0)
    meta[...] = (weight_of + named).astype(BF16)

    pl.semaphore_wait(barrier, len(greet))

    put(meta, xmeta, xss.at[NCH, 0], xrs.at[NCH, 0], xfar).start()

    def xchunk(j):
        col = chunk_col(jnp.int32(j))
        put(tk.at[:, pl.ds(col, CH)], xr.at[j, :, pl.ds(0, CH)], xss.at[j, 0], xrs.at[j, 0], xfar).start()
        put(og.at[:, pl.ds(col, CH)], xr.at[j, :, pl.ds(CH, CH)], xss.at[j, 1], xrs.at[j, 1], xfar).start()

    w_all = (wg, wu, wd)

    def shard(n, src, dst, to):
        put(w_all[n].at[src], w_all[n].at[dst], ags.at[dst, n, 0], agr.at[dst, n, 0], to).start()

    def half(n, src, dst, h, to):
        size = w_all[n].shape[1] // 2
        rows = pl.ds(h * size, size)
        put(
            w_all[n].at[src, rows], w_all[n].at[dst, rows], ags.at[dst, n, h], agr.at[dst, n, h], to
        ).start()

    for n in range(3):
        shard(n, 0, 2, yup)
        shard(n, 0, 1, ydn)
    xchunk(0)
    xchunk(1)
    shard(0, 0, 4, xnear)
    xchunk(2)
    shard(1, 0, 4, xnear)
    xchunk(3)
    shard(2, 0, 4, xnear)
    for j in range(4, NCH):
        xchunk(j)

    before = (
        lax.broadcasted_iota(jnp.int32, (T, T), 0) < lax.broadcasted_iota(jnp.int32, (T, T), 1)
    ).astype(BF16)
    same = (
        lax.broadcasted_iota(jnp.int32, (T, T), 0) == lax.broadcasted_iota(jnp.int32, (T, T), 1)
    ).astype(BF16)

    def tables(src, first, g, gt, which):
        table = src[...]
        listed, rank = tn(table, same), tn(table, before)
        slots[which] = jnp.where(listed > 0.5, rank + first, -1.0)
        slot_id = lax.broadcasted_iota(jnp.int32, (RB, T), 0).astype(F32)

        def one(b, _):
            row = slots[which, pl.ds(16 + x_hi * 8 + b, 1), :]
            hot = jnp.where(slot_id == row, 1.0, 0.0)
            g[b] = hot.astype(BF16)
            gt[:, pl.ds(pl.multiple_of(b * RB, RB), RB)] = hot.T.astype(BF16)
            return 0

        lax.fori_loop(0, NB, one, 0)

    tables(meta, 0.0, go, gto, 0)
    got(xmeta, xrs.at[NCH, 0])
    tables(xmeta, float(CAP), gp, gtp, 1)

    rows_sent = pl.ds(0, RV)

    def to_peers(start, own, zz):
        for cc in range(2):
            b = zz * 2 + cc

            @pl.when(b != me)
            def _():
                start(b)

            @pl.when(b == me)
            def _():
                own(b)

    def weights_table(m, _):
        zz = rem(z + 1 + m, 4)
        two = pl.ds(zz * 2, 2)
        picked = nn(go[two].reshape(2 * RB, T), meta[...]) + nn(
            gp[two].reshape(2 * RB, T), xmeta[...]
        )
        zms[two] = picked.astype(BF16).reshape(2, RB, 128)

        def start(b):
            put(
                zms.at[b, rows_sent], zmr.at[me, rows_sent], zss.at[NCH], zrs.at[NCH], peer(b)
            ).start()

        def own(b):
            zmr[b] = zms[b]

        to_peers(start, own, zz)
        return 0

    lax.fori_loop(0, 4, weights_table, 0)

    seven = pl.ds(0, NB - 1)

    def forward_phase(ag, au, ah):
        def reset(m, _):
            rows = pl.ds(pl.multiple_of(m * RB, RB), RB)
            ag[rows] = jnp.zeros((RB, FF), F32)
            au[rows] = jnp.zeros((RB, FF), F32)
            ah[rows] = jnp.zeros((RB, FF), F32)
            return 0

        lax.fori_loop(0, NB, reset, 0)

        def produce(j):
            slot = rem(j, 2)
            col = chunk_col(j)
            got(xr.at[j, :, pl.ds(0, CH)], xrs.at[j, 0])
            got(xr.at[j, :, pl.ds(CH, CH)], xrs.at[j, 1])

            @pl.when(j >= 2)
            def _():
                sent(zs.at[slot, seven, rows_sent], zss.at[j - 2])

            def gather(m, _):
                zz = rem(z + 1 + m, 4)
                two = pl.ds(zz * 2, 2)
                mine, theirs = go[two].reshape(2 * RB, T), gp[two].reshape(2 * RB, T)
                rows_t = nn(mine, tk[:, pl.ds(col, CH)]) + nn(theirs, xr[j, :, :CH])
                zs[slot, two, :, :CH] = rows_t.astype(BF16).reshape(2, RB, CH)
                rows_g = nn(mine, og[:, pl.ds(col, CH)]) + nn(theirs, xr[j, :, CH:])
                zs[slot, two, :, CH:] = rows_g.astype(BF16).reshape(2, RB, CH)

                def start(b):
                    put(
                        zs.at[slot, b, rows_sent], zr.at[j, me, rows_sent],
                        zss.at[j], zrs.at[j], peer(b),
                    ).start()

                def own(b):
                    zr[j, b] = zs[slot, b]

                to_peers(start, own, zz)
                return 0

            lax.fori_loop(0, 4, gather, 0)

        def got_shard(idx):
            for n in range(3):
                got(w_all[n].at[idx], agr.at[idx, n, 0])

        def got_halves(idx):
            for n in range(3):
                size = w_all[n].shape[1] // 2
                for h in range(2):
                    got(w_all[n].at[idx, pl.ds(h * size, size)], agr.at[idx, n, h])

        def consume(j):
            @pl.when(j == 1)
            def _():
                got_shard(1)
                got_shard(2)
                for n in range(3):
                    half(n, 1, 3, 1, ydn)
                    half(n, 2, 3, 0, yup)

            @pl.when(j == 3)
            def _():
                got_halves(3)
                got_shard(4)
                for n in range(3):
                    shard(n, 4, 6, yup)
                    shard(n, 4, 5, ydn)

            @pl.when(j == 5)
            def _():
                got_shard(5)
                got_shard(6)
                for n in range(3):
                    half(n, 5, 7, 1, ydn)
                    half(n, 6, 7, 0, yup)

            @pl.when(j == 7)
            def _():
                got_halves(7)

            got(zr.at[j, seven, rows_sent], zrs.at[j])

            def tile(m, _):
                block = zr[j, pl.ds(m * 2, 2)].reshape(2 * RB, 2 * CH)
                rows = pl.ds(pl.multiple_of(m * 2 * RB, 2 * RB), 2 * RB)
                ag[rows] += nn(block[:, :CH], wg[j])
                au[rows] += nn(block[:, :CH], wu[j])
                ah[rows] += nt(block[:, CH:], wd[j])
                return 0

            lax.fori_loop(0, 4, tile, 0)

        def step(j, _):
            @pl.when(j < NCH)
            def _():
                produce(j)

            @pl.when(j > 0)
            def _():
                consume(j - 1)

            return 0

        lax.fori_loop(0, NCH + 1, step, 0)

        got(zmr.at[seven, rows_sent], zrs.at[NCH])
        lane_of = lax.broadcasted_iota(jnp.int32, (RB, 128), 1)

        def delta(b, _):
            rows = pl.ds(pl.multiple_of(b * RB, RB), RB)
            weight = jnp.sum(
                jnp.where(lane_of == ex, zmr[b].astype(F32), 0.0), axis=1, keepdims=True
            )
            gate, up, back = ag[rows], au[rows], ah[rows]
            sig = jax.nn.sigmoid(gate)
            act = gate * sig
            hidden = (act * up).astype(BF16).astype(F32)
            dot = jnp.sum(hidden * back, axis=1, keepdims=True)
            zds[b] = jnp.where(lane_of == ex, dot, 0.0).astype(BF16)
            back = back * weight
            gd[rows] = (back * up * sig * (1.0 + gate * (1.0 - sig))).astype(BF16)
            ud[rows] = (back * act).astype(BF16)
            hwt[:, rows] = (hidden * weight).T.astype(BF16)
            return 0

        lax.fori_loop(0, NB, delta, 0)

    acc = pltpu.VMEM((ROWS, FF), F32)
    pl.run_scoped(forward_phase, acc, acc, acc)

    sent(meta, xss.at[NCH, 0])
    for j in range(NCH):
        sent(xr.at[j, :, pl.ds(0, CH)], xss.at[j, 0])
        sent(xr.at[j, :, pl.ds(CH, CH)], xss.at[j, 1])
    sent(zms.at[seven, rows_sent], zss.at[NCH])
    for j in (NCH - 2, NCH - 1):
        sent(zs.at[j % 2, seven, rows_sent], zss.at[j])

    def backward_phase(pg, pu, pd):
        p_all, ra, rb = (pg, pu, pd), (rag, rau, rad), (rbg, rbu, rbd)
        rx, outs = (rxg, rxu, rxd), (gate_out, up_out, down_out)

        def send_dots(b, _):
            @pl.when(b != me)
            def _():
                put(
                    zds.at[b, rows_sent], rdot.at[me, rows_sent], zts.at[NCH], ztr.at[NCH], peer(b)
                ).start()

            @pl.when(b == me)
            def _():
                rdot[b] = zds[b]

            return 0

        lax.fori_loop(0, NB, send_dots, 0)

        def index_of(q):
            ge2, ge6 = quo(q + 6, 8), quo(q + 2, 8)
            r = q + 6
            mid = 4 * (1 - (quo(r, 2) - 4)) + 1 + rem(r, 2)
            return (1 - ge2) * (7 - 4 * q) + (ge2 - ge6) * mid + ge6 * (4 * (7 - q))

        def compute(q):
            idx = index_of(q)
            slot, lanes = rem(quo(q, 2), 2), pl.ds(pl.multiple_of(rem(q, 2) * CH, CH), CH)

            @pl.when(q >= 4)
            def _():
                sent(zs.at[slot, seven, rows_sent, lanes], zts.at[q - 4])

            def input_rows(m, _):
                zz = rem(z + 1 + m, 4)
                rows = pl.ds(pl.multiple_of(zz * 2 * RB, 2 * RB), 2 * RB)
                out = nt(gd[rows], wg[idx]) + nt(ud[rows], wu[idx])
                zs[slot, pl.ds(zz * 2, 2), :, lanes] = out.astype(BF16).reshape(2, RB, CH)

                def start(b):
                    put(
                        zs.at[slot, b, rows_sent, lanes], ret.at[q, me, rows_sent],
                        zts.at[q], ztr.at[q], peer(b),
                    ).start()

                def own(b):
                    ret[q, b] = zs[slot, b, :, lanes]

                to_peers(start, own, zz)
                return 0

            lax.fori_loop(0, 4, input_rows, 0)
            toks = zr[idx, :, :, :CH].reshape(ROWS, CH)
            pg[q] = tn(toks, gd[...]).astype(BF16)
            pu[q] = tn(toks, ud[...]).astype(BF16)
            pd[q] = nn(hwt[...], zr[idx, :, :, CH:].reshape(ROWS, CH)).astype(BF16)

        def send_far(q, l):
            for n in range(3):
                size = p_all[n].shape[1] // 2
                for h in range(2):
                    put(
                        p_all[n].at[q, pl.ds(h * size, size)], ra[n].at[l, h],
                        ras.at[l, h, n], rar.at[l, h, n], ydir[h],
                    ).start()

        def send_near(q, l):
            for n in range(3):
                size = p_all[n].shape[1] // 2
                for h in range(2):
                    got(ra[n].at[l, h], rar.at[l, h, n])
                    rows = pl.ds(h * size, size)
                    p_all[n][q + h, rows] = (
                        p_all[n][q + h, rows].astype(F32) + ra[n][l, h].astype(F32)
                    ).astype(BF16)
                    put(
                        p_all[n].at[q + h], rb[n].at[l, h], rbs.at[l, h, n], rbr.at[l, h, n], ydir[h]
                    ).start()

        def gathered(q, l, n):
            for h in range(2):
                got(rb[n].at[l, h], rbr.at[l, h, n])
            return p_all[n][q].astype(F32) + rb[n][l, 0].astype(F32) + rb[n][l, 1].astype(F32)

        def back_rows(q):
            got(ret.at[q, seven, rows_sent], ztr.at[q])
            col = chunk_col(index_of(q))
            rows = ret[q].reshape(ROWS, CH)
            pown[q] = nn(gto[...], rows)
            og[:, pl.ds(col, CH)] = nn(gtp[...], rows).astype(BF16)
            put(og.at[:, pl.ds(col, CH)], xr2.at[q], xts.at[q], xtr.at[q], xfar).start()

        def step(q, _):
            compute(q)
            for l in (1, 0):

                @pl.when(q == 1 - l)
                def _():
                    send_far(1 - l, l)

                @pl.when(q == 5 - 2 * l)
                def _():
                    send_near(4 - 2 * l, l)

            @pl.when(q >= 4)
            def _():
                back_rows(q - 4)

            return 0

        lax.fori_loop(0, NCH, step, 0)

        def step_b(q, _):
            back_rows(q)
            return 0

        lax.fori_loop(4, NCH, step_b, 0)

        got(rdot.at[seven, rows_sent], ztr.at[NCH])
        dots = rdot[...].reshape(ROWS, 128)
        ddown[...] = nn(gto[...], dots)
        dpar[...] = nn(gtp[...], dots).astype(BF16)
        put(dpar, xdot, xts.at[NCH], xtr.at[NCH], xfar).start()

        for n in range(3):
            p_all[n][6] = gathered(6, 1, n).astype(BF16)
            put(p_all[n].at[6], rx[n], rxs.at[n], rxr.at[n], xnear).start()

        def finish(q, _):
            got(xr2.at[q], xtr.at[q])
            col = chunk_col(index_of(q))
            tk[:, pl.ds(col, CH)] = (pown[q] + xr2[q].astype(F32)).astype(BF16)
            return 0

        lax.fori_loop(0, NCH, finish, 0)
        whole = pltpu.make_async_copy(tk, token_out, osem.at[3])
        whole.start()
        got(xdot, xtr.at[NCH])
        all_dots = ddown[...] + xdot[...].astype(F32)
        lane_t = lax.broadcasted_iota(jnp.int32, (T, 128), 1)
        first = jnp.sum(jnp.where(lane_t == ids[:, 0:1], all_dots, 0.0), axis=1, keepdims=True)
        second = jnp.sum(jnp.where(lane_t == ids[:, 1:2], all_dots, 0.0), axis=1, keepdims=True)
        pick = lax.broadcasted_iota(jnp.int32, (T, 2), 1)
        route_out[...] = jnp.where(pick == 0, first, second).astype(BF16)

        last = [whole]
        for n in range(3):
            total = gathered(7, 0, n)
            got(rx[n], rxr.at[n])
            p_all[n][7] = (total + rx[n][...].astype(F32)).astype(BF16)
            cp = pltpu.make_async_copy(p_all[n].at[7], outs[n], osem.at[n])
            cp.start()
            last.append(cp)

        for idx in (1, 2, 4, 5, 6):
            for n in range(3):
                sent(w_all[n].at[idx], ags.at[idx, n, 0])
        for n in range(3):
            size = w_all[n].shape[1] // 2
            for h in range(2):
                for idx in (3, 7):
                    sent(w_all[n].at[idx, pl.ds(h * size, size)], ags.at[idx, n, h])
                for l in range(2):
                    sent(ra[n].at[l, h], ras.at[l, h, n])
                    sent(rb[n].at[l, h], rbs.at[l, h, n])
            sent(rx[n], rxs.at[n])
        sent(zds.at[seven, rows_sent], zts.at[NCH])
        for q in range(4, NCH):
            sent(zs.at[0, seven, rows_sent, pl.ds(0, CH)], zts.at[q])
        for q in range(NCH):
            sent(xr2.at[q], xts.at[q])
        sent(dpar, xts.at[NCH])
        for cp in last:
            cp.wait()

    pl.run_scoped(
        backward_phase,
        pltpu.VMEM((NCH, CH, FF), BF16),
        pltpu.VMEM((NCH, CH, FF), BF16),
        pltpu.VMEM((NCH, FF, CH), BF16),
    )


def on_device(tokens, out_grad, expert_ids, route_weight, w_gate, w_up, w_down):
    hbm = pl.BlockSpec(memory_space=pltpu.HBM)
    vmem = pltpu.VMEM
    sem = pltpu.SemaphoreType.DMA
    outs = pl.pallas_call(
        kernel,
        out_shape=(
            jax.ShapeDtypeStruct((T, D), BF16),
            jax.ShapeDtypeStruct((T, 2), BF16),
            jax.ShapeDtypeStruct((CH, FF), BF16),
            jax.ShapeDtypeStruct((CH, FF), BF16),
            jax.ShapeDtypeStruct((FF, CH), BF16),
        ),
        in_specs=[hbm] * 7,
        out_specs=(hbm, pl.BlockSpec(memory_space=vmem), hbm, hbm, hbm),
        scratch_shapes=[
            vmem((T, D), BF16), vmem((T, D), BF16), vmem((T, 2), jnp.int32), vmem((T, 2), BF16),
            vmem((T, 128), BF16), vmem((T, 128), BF16), vmem((NCH, T, 2 * CH), BF16),
            vmem((2, 128, T), F32), vmem((NB, RB, T), BF16), vmem((NB, RB, T), BF16),
            vmem((T, ROWS), BF16), vmem((T, ROWS), BF16),
            vmem((2, NB, RB, 2 * CH), BF16), vmem((NCH, NB, RB, 2 * CH), BF16),
            vmem((NB, RB, 128), BF16), vmem((NB, RB, 128), BF16),
            vmem((NCH, CH, FF), BF16), vmem((NCH, CH, FF), BF16), vmem((NCH, FF, CH), BF16),
            vmem((ROWS, FF), BF16), vmem((ROWS, FF), BF16), vmem((FF, ROWS), BF16),
            vmem((2, 2, CH // 2, FF), BF16), vmem((2, 2, CH // 2, FF), BF16),
            vmem((2, 2, FF // 2, CH), BF16),
            vmem((2, 2, CH, FF), BF16), vmem((2, 2, CH, FF), BF16), vmem((2, 2, FF, CH), BF16),
            vmem((CH, FF), BF16), vmem((CH, FF), BF16), vmem((FF, CH), BF16),
            vmem((NCH, NB, RB, CH), BF16), vmem((NB, RB, 128), BF16), vmem((NB, RB, 128), BF16),
            vmem((NCH, T, CH), F32), vmem((NCH, T, CH), BF16),
            vmem((T, 128), F32), vmem((T, 128), BF16), vmem((T, 128), BF16),
            sem((7,)), sem((4,)), sem((NCH + 1, 2)), sem((NCH + 1, 2)),
            sem((NCH + 1,)), sem((NCH + 1,)), sem((NCH, 3, 2)), sem((NCH, 3, 2)),
            sem((NCH + 1,)), sem((NCH + 1,)), sem((NCH + 1,)), sem((NCH + 1,)),
            sem((2, 2, 3)), sem((2, 2, 3)), sem((2, 2, 3)), sem((2, 2, 3)), sem((3,)), sem((3,)),
        ],
        compiler_params=pltpu.CompilerParams(
            collective_id=0, has_side_effects=True, vmem_limit_bytes=67043328
        ),
        name="routed_backward",
    )(
        tokens, out_grad, expert_ids, route_weight,
        w_gate.reshape(CH, FF), w_up.reshape(CH, FF), w_down.reshape(FF, CH),
    )
    token_grad, route_grad, gate, up, down = outs
    return token_grad, route_grad, gate[None], up[None], down[None]


def solution(mesh):
    placed = (
        P(("dp", "expert"), None),
        P(("dp", "expert"), None),
        P(("dp", "expert"), None),
        P(("dp", "expert"), None),
        P("expert", "dp", None),
        P("expert", "dp", None),
        P("expert", None, "dp"),
    )
    return jax.shard_map(
        on_device,
        mesh=mesh,
        in_specs=placed,
        out_specs=(
            P(("dp", "expert"), None),
            P(("dp", "expert"), None),
            P("expert", "dp", None),
            P("expert", "dp", None),
            P("expert", None, "dp"),
        ),
        check_vma=False,
    )
```
